32 devices in a mesh: lat: 8 (over y, x, core), lon: 4 (over z).
Axes of the slice: x: 2, y: 2, z: 4, core: 2. Of those that a mesh axis runs over, the one named last changes fastest.
Arguments:
- pressure: float32 [256, 128, 128], P('lat', 'lon'), may hold values from 0.2 to 1.8
- earlier: float32 [256, 128, 128], P('lat', 'lon'), may hold values from 0.2 to 1.8
- speed_square: float32 [256, 128, 128], P('lat', 'lon'), may hold values from 0.05 to 0.4
Outputs:
- potential: float32 [256, 128, 128], P('lat', 'lon')
- pressure_end: float32 [256, 128, 128], P('lat', 'lon')
The draws below stay inside these ranges and needn't reach their ends.
All inputs are finite; a program needn't handle non-finite values.
Results may differ from the reference program's by a relative error of at most 0.00002.
Values sent between devices are 32-bit elements; how exact they have to be, the bound alone decides.
A program may use at most 64 MiB of HBM per device.

```python
import jax
import jax.numpy as jnp
from jax import lax

GRID_Y = 256
GRID_X = 128
MEMBERS = 128
STEPS = 4


def block_scale(stream_key, shape, cuts, smallest, largest):
    factor_of = 1.0
    for dim, blocks in cuts:
        draws = jax.random.uniform(jax.random.fold_in(jax.random.fold_in(stream_key, 6), dim), (blocks,), jnp.float32, smallest / len(cuts), largest / len(cuts))
        factor_of = factor_of * jnp.repeat(jnp.exp(draws), shape[dim] // blocks).reshape((-1,) + (1,) * (len(shape) - 1 - dim))
    return factor_of


def setup_inputs(seed: int = 0) -> dict:
    seeds = jax.random.split(jax.random.key(seed), 4)
    pressure = jnp.clip(0.2 + 1.5999999 * jax.random.uniform(seeds[0], (GRID_Y, GRID_X, MEMBERS), jnp.float32) ** block_scale(seeds[0], (GRID_Y, GRID_X, MEMBERS), ((0, 8), (1, 4)), -0.2, 0.2), 0.2, 1.8)
    earlier = jnp.clip(0.2 + 1.5999999 * jax.random.uniform(seeds[1], (GRID_Y, GRID_X, MEMBERS), jnp.float32) ** block_scale(seeds[1], (GRID_Y, GRID_X, MEMBERS), ((0, 8), (1, 4)), -0.2, 0.2), 0.2, 1.8)
    speed_square = jnp.clip(0.05 + 0.35 * jax.random.uniform(seeds[2], (GRID_Y, GRID_X, MEMBERS), jnp.float32) ** block_scale(seeds[2], (GRID_Y, GRID_X, MEMBERS), ((0, 8), (1, 4)), -0.2, 0.2), 0.05, 0.4)
    return {"pressure": pressure, "earlier": earlier, "speed_square": speed_square}


def strip_edges(values, dims):
    for dim in dims:
        values = lax.slice_in_dim(values, 1, values.shape[dim] - 1, axis=dim)
    return values


def neighbour(values, dim, start, dims):
    others = [other for other in dims if other != dim]
    values = strip_edges(values, others)
    return lax.slice_in_dim(values, start, start + values.shape[dim] - 2, axis=dim)


def one_step(padded, before, speed_square):
    middle = strip_edges(padded, (0, 1))
    lower = [neighbour(padded, dim, 0, (0, 1)) for dim in (0, 1)]
    upper = [neighbour(padded, dim, 2, (0, 1)) for dim in (0, 1)]
    spread = lower[0] + upper[0] + lower[1] + upper[1] - 4.0 * middle
    return 2.0 * middle - before + speed_square * spread


def reference(pressure, earlier, speed_square):
    for step in range(STEPS):
        later = one_step(jnp.pad(pressure, ((1, 1), (1, 1), (0, 0)), mode="constant"), earlier, speed_square)
        earlier, pressure = pressure, later
    potential = jnp.cumsum(pressure, axis=0) / GRID_Y
    return potential, pressure
```

```python
import functools

import jax
import jax.numpy as jnp
from jax import lax
from jax.experimental import pallas as pl
from jax.experimental.pallas import tpu as pltpu
from jax.sharding import PartitionSpec as P

STEPS = 4
PAD = 8
MESH = pl.DeviceIdType.MESH


def corner_cells():
    cells = [(0, i, j) for i in range(STEPS - 1) for j in range(STEPS - 1 - i)]
    for array in (1, 2):
        cells += [(array, i, j) for i in range(STEPS - 2) for j in range(STEPS - 2 - i)]
    return cells


def kernel(
    n_lat, n_lon, p_in, e_in, c_in, pot_out, end_out,
    p, e, c, lon_send, lon_recv, corner_send, corner_recv, here, totals, below,
    load_sem, store_sem, lat_sems, lon_sems, corner_sems, total_send_sem, total_recv_sem,
):
    rows, cols = p_in.shape[0], p_in.shape[1]
    fields = (p, e, c)
    depth = (STEPS, STEPS - 1, STEPS - 1)
    top, left = STEPS, PAD
    bottom, right = top + rows, left + cols
    me_lat, me_lon = lax.axis_index("lat"), lax.axis_index("lon")
    has_lat = (me_lat > 0, me_lat < n_lat - 1)
    has_lon = (me_lon > 0, me_lon < n_lon - 1)
    step_of = (-1, 1)

    loads = []
    for k, (src, dst) in enumerate(zip((p_in, e_in, c_in), fields)):
        copy = pltpu.make_async_copy(src, dst.at[top:bottom, left:right], load_sem.at[k])
        copy.start()
        loads.append(copy)

    barrier = pltpu.get_barrier_semaphore()

    def greet(lat, lon):
        pl.semaphore_signal(
            barrier, inc=1, device_id={"lat": lat, "lon": lon}, device_id_type=MESH
        )

    for a in range(2):
        for b in range(2):
            @pl.when(has_lat[a] & has_lon[b])
            def _():
                greet(me_lat + step_of[a], me_lon + step_of[b])
    for b in range(2):
        @pl.when(has_lon[b])
        def _():
            greet(me_lat, me_lon + step_of[b])
    for j in range(n_lat):
        @pl.when(me_lat != j)
        def _():
            greet(j, me_lon)

    zero = jnp.int32(0)
    one = jnp.int32(1)
    count_lat = sum(jnp.where(h, one, zero) for h in has_lat)
    count_lon = sum(jnp.where(h, one, zero) for h in has_lon)
    peers = n_lat - 1 + count_lon + count_lon * count_lat

    for a in range(2):
        @pl.when(jnp.logical_not(has_lat[a]))
        def _():
            for f in fields:
                start = 0 if a == 0 else bottom
                f[start:start + STEPS] = jnp.zeros((STEPS,) + f.shape[1:], f.dtype)
    for b in range(2):
        @pl.when(jnp.logical_not(has_lon[b]))
        def _():
            for f in fields:
                start = 0 if b == 0 else right
                f[:, start:start + PAD] = jnp.zeros((f.shape[0], PAD, f.shape[2]), f.dtype)

    for copy in loads:
        copy.wait()

    for b in range(2):
        @pl.when(has_lon[b])
        def _():
            base = 0
            for f, d in zip(fields, depth):
                start = left if b == 0 else right - d
                for r in range(rows):
                    lon_send[b, base + r * d:base + (r + 1) * d] = f[top + r, start:start + d]
                base += rows * d
    cells = corner_cells()
    for a in range(2):
        for b in range(2):
            @pl.when(has_lat[a] & has_lon[b])
            def _():
                for k, (which, i, j) in enumerate(cells):
                    r = top + i if a == 0 else bottom - 1 - i
                    s = left + j if b == 0 else right - 1 - j
                    corner_send[2 * a + b, k:k + 1] = fields[which][r, s:s + 1]

    pl.semaphore_wait(barrier, peers)

    def corner_copy(a, b):
        return pltpu.make_async_remote_copy(
            src_ref=corner_send.at[2 * a + b],
            dst_ref=corner_recv.at[2 * (1 - a) + 1 - b],
            send_sem=corner_sems.at[0, 2 * a + b],
            recv_sem=corner_sems.at[1, 2 * (1 - a) + 1 - b],
            device_id={"lat": me_lat + step_of[a], "lon": me_lon + step_of[b]},
            device_id_type=MESH,
        )

    def lon_copy(b):
        return pltpu.make_async_remote_copy(
            src_ref=lon_send.at[b],
            dst_ref=lon_recv.at[1 - b],
            send_sem=lon_sems.at[0, b],
            recv_sem=lon_sems.at[1, 1 - b],
            device_id={"lat": me_lat, "lon": me_lon + step_of[b]},
            device_id_type=MESH,
        )

    def lat_copy(a, k):
        f, d = fields[k], depth[k]
        src = top if a == 0 else bottom - d
        dst = bottom if a == 0 else top - d
        return pltpu.make_async_remote_copy(
            src_ref=f.at[src:src + d, left:right],
            dst_ref=f.at[dst:dst + d, left:right],
            send_sem=lat_sems.at[0, a, k],
            recv_sem=lat_sems.at[1, 1 - a, k],
            device_id={"lat": me_lat + step_of[a], "lon": me_lon},
            device_id_type=MESH,
        )

    for a in range(2):
        for b in range(2):
            @pl.when(has_lat[a] & has_lon[b])
            def _():
                corner_copy(a, b).start()
    for b in range(2):
        @pl.when(has_lon[b])
        def _():
            lon_copy(b).start()
    for a in range(2):
        @pl.when(has_lat[a])
        def _():
            for k in range(3):
                lat_copy(a, k).start()

    for a in range(2):
        for b in range(2):
            @pl.when(has_lat[a] & has_lon[b])
            def _():
                corner_copy(1 - a, 1 - b).wait_recv()
                corner_copy(a, b).wait_send()
                for k, (which, i, j) in enumerate(cells):
                    r = top - 1 - i if a == 0 else bottom + i
                    s = left - 1 - j if b == 0 else right + j
                    fields[which][r, s:s + 1] = corner_recv[2 * a + b, k:k + 1]
    for b in range(2):
        @pl.when(has_lon[b])
        def _():
            lon_copy(1 - b).wait_recv()
            lon_copy(b).wait_send()
            base = 0
            for f, d in zip(fields, depth):
                start = left - d if b == 0 else right
                for r in range(rows):
                    f[top + r, start:start + d] = lon_recv[b, base + r * d:base + (r + 1) * d]
                base += rows * d
    for a in range(2):
        @pl.when(has_lat[a])
        def _():
            for k in range(3):
                lat_copy(1 - a, k).wait_recv()
                lat_copy(a, k).wait_send()

    now, old = p, e
    for step in range(STEPS):
        margin = STEPS - 1 - step
        lo, hi = left - margin, right + margin
        last = step == STEPS - 1

        def one_row(r, total, now=now, old=old, lo=lo, hi=hi, last=last):
            middle = now[r, lo:hi]
            spread = (
                now[r - 1, lo:hi] + now[r + 1, lo:hi]
                + now[r, lo - 1:hi - 1] + now[r, lo + 1:hi + 1] - 4.0 * middle
            )
            later = 2.0 * middle - old[r, lo:hi] + c[r, lo:hi] * spread
            old[r, lo:hi] = later
            if last:
                total = total + later
                here[r - top] = total
            return total

        start = jnp.zeros((cols, p.shape[2]), p.dtype) if last else 0
        total = lax.fori_loop(top - margin, bottom + margin, one_row, start, unroll=2)
        now, old = old, now
    below[...] = total

    def total_copy(j):
        return pltpu.make_async_remote_copy(
            src_ref=below,
            dst_ref=totals.at[me_lat],
            send_sem=total_send_sem.at[j],
            recv_sem=total_recv_sem.at[me_lat],
            device_id={"lat": j, "lon": me_lon},
            device_id_type=MESH,
        )

    def total_arrival(j):
        return pltpu.make_async_remote_copy(
            src_ref=below,
            dst_ref=totals.at[j],
            send_sem=total_send_sem.at[j],
            recv_sem=total_recv_sem.at[j],
            device_id={"lat": j, "lon": me_lon},
            device_id_type=MESH,
        )

    for j in reversed(range(1, n_lat)):
        @pl.when(me_lat < j)
        def _():
            total_copy(j).start()
    end_copy = pltpu.make_async_copy(
        now.at[top:bottom, left:right], end_out, store_sem.at[0]
    )
    end_copy.start()

    def arrive(j, acc):
        total_arrival(j).wait_recv()
        return acc + totals[j]

    before = lax.fori_loop(0, me_lat, arrive, jnp.zeros((cols, p.shape[2]), p.dtype))
    scale = 1.0 / (rows * n_lat)

    def finish(r, carry):
        here[r] = (here[r] + before) * scale
        return carry

    lax.fori_loop(0, rows, finish, 0, unroll=4)
    pot_copy = pltpu.make_async_copy(here, pot_out, store_sem.at[1])
    pot_copy.start()
    for j in range(1, n_lat):
        @pl.when(me_lat < j)
        def _():
            total_copy(j).wait_send()
    end_copy.wait()
    pot_copy.wait()


def on_device(n_lat, n_lon, pressure, earlier, speed_square):
    rows, cols, members = pressure.shape
    packed = rows * (3 * STEPS - 2)
    corner_rows = -(-len(corner_cells()) // 8) * 8
    f32 = jnp.float32
    wide = pltpu.VMEM((rows + 2 * STEPS, cols + 2 * PAD, members), f32)
    any_space = pl.BlockSpec(memory_space=pl.ANY)
    dma = pltpu.SemaphoreType.DMA
    return pl.pallas_call(
        functools.partial(kernel, n_lat, n_lon),
        out_shape=[jax.ShapeDtypeStruct(pressure.shape, f32)] * 2,
        in_specs=[any_space] * 3,
        out_specs=[any_space] * 2,
        scratch_shapes=[
            wide, wide, wide,
            pltpu.VMEM((2, packed, members), f32),
            pltpu.VMEM((2, packed, members), f32),
            pltpu.VMEM((4, corner_rows, members), f32),
            pltpu.VMEM((4, corner_rows, members), f32),
            pltpu.VMEM((rows, cols, members), f32),
            pltpu.VMEM((n_lat, cols, members), f32),
            pltpu.VMEM((cols, members), f32),
            dma((3,)), dma((2,)), dma((2, 2, 3)), dma((2, 2)), dma((2, 4)),
            dma((n_lat,)), dma((n_lat,)),
        ],
        compiler_params=pltpu.CompilerParams(collective_id=0, has_side_effects=True),
        name="waves",
    )(pressure, earlier, speed_square)


def solution(mesh):
    spec = P("lat", "lon", None)
    body = functools.partial(on_device, mesh.shape["lat"], mesh.shape["lon"])
    return jax.shard_map(
        body, mesh=mesh, in_specs=(spec,) * 3, out_specs=(spec,) * 2, check_vma=False
    )
```

```python
import functools

import jax
import jax.numpy as jnp
from jax import lax
from jax.experimental import pallas as pl
from jax.experimental.pallas import tpu as pltpu
from jax.sharding import PartitionSpec as P

STEPS = 4
PAD = 8
MESH = pl.DeviceIdType.MESH


def corner_cells():
    cells = [(0, i, j) for i in range(STEPS - 1) for j in range(STEPS - 1 - i)]
    for array in (1, 2):
        cells += [(array, i, j) for i in range(STEPS - 2) for j in range(STEPS - 2 - i)]
    return cells


def kernel(
    n_lat, n_lon, p_in, e_in, c_in, here, end, before,
    p, e, c, lon_send, lon_recv, corner_send, corner_recv, totals, below,
    load_sem, lat_sems, lon_sems, corner_sems, total_send_sem, total_recv_sem,
):
    rows, cols = p_in.shape[0], p_in.shape[1]
    fields = (p, e, c)
    depth = (STEPS, STEPS - 1, STEPS - 1)
    top, left = STEPS, PAD
    bottom, right = top + rows, left + cols
    me_lat, me_lon = lax.axis_index("lat"), lax.axis_index("lon")
    has_lat = (me_lat > 0, me_lat < n_lat - 1)
    has_lon = (me_lon > 0, me_lon < n_lon - 1)
    step_of = (-1, 1)

    loads = []
    for k, (src, dst) in enumerate(zip((p_in, e_in, c_in), fields)):
        copy = pltpu.make_async_copy(src, dst.at[top:bottom, left:right], load_sem.at[k])
        copy.start()
        loads.append(copy)

    barrier = pltpu.get_barrier_semaphore()

    def greet(lat, lon):
        pl.semaphore_signal(
            barrier, inc=1, device_id={"lat": lat, "lon": lon}, device_id_type=MESH
        )

    for a in range(2):
        for b in range(2):
            @pl.when(has_lat[a] & has_lon[b])
            def _():
                greet(me_lat + step_of[a], me_lon + step_of[b])
    for b in range(2):
        @pl.when(has_lon[b])
        def _():
            greet(me_lat, me_lon + step_of[b])
    for j in range(n_lat):
        @pl.when(me_lat != j)
        def _():
            greet(j, me_lon)

    zero = jnp.int32(0)
    one = jnp.int32(1)
    count_lat = sum(jnp.where(h, one, zero) for h in has_lat)
    count_lon = sum(jnp.where(h, one, zero) for h in has_lon)
    peers = n_lat - 1 + count_lon + count_lon * count_lat

    for a in range(2):
        @pl.when(jnp.logical_not(has_lat[a]))
        def _():
            for f in fields:
                start = 0 if a == 0 else bottom
                f[start:start + STEPS] = jnp.zeros((STEPS,) + f.shape[1:], f.dtype)
    for b in range(2):
        @pl.when(jnp.logical_not(has_lon[b]))
        def _():
            for f in fields:
                start = 0 if b == 0 else right
                f[:, start:start + PAD] = jnp.zeros((f.shape[0], PAD, f.shape[2]), f.dtype)

    for copy in loads:
        copy.wait()

    for b in range(2):
        @pl.when(has_lon[b])
        def _():
            base = 0
            for f, d in zip(fields, depth):
                start = left if b == 0 else right - d
                for r in range(rows):
                    lon_send[b, base + r * d:base + (r + 1) * d] = f[top + r, start:start + d]
                base += rows * d
    cells = corner_cells()
    for a in range(2):
        for b in range(2):
            @pl.when(has_lat[a] & has_lon[b])
            def _():
                for k, (which, i, j) in enumerate(cells):
                    r = top + i if a == 0 else bottom - 1 - i
                    s = left + j if b == 0 else right - 1 - j
                    corner_send[2 * a + b, k:k + 1] = fields[which][r, s:s + 1]

    pl.semaphore_wait(barrier, peers)

    def corner_copy(a, b):
        return pltpu.make_async_remote_copy(
            src_ref=corner_send.at[2 * a + b],
            dst_ref=corner_recv.at[2 * (1 - a) + 1 - b],
            send_sem=corner_sems.at[0, 2 * a + b],
            recv_sem=corner_sems.at[1, 2 * (1 - a) + 1 - b],
            device_id={"lat": me_lat + step_of[a], "lon": me_lon + step_of[b]},
            device_id_type=MESH,
        )

    def lon_copy(b):
        return pltpu.make_async_remote_copy(
            src_ref=lon_send.at[b],
            dst_ref=lon_recv.at[1 - b],
            send_sem=lon_sems.at[0, b],
            recv_sem=lon_sems.at[1, 1 - b],
            device_id={"lat": me_lat, "lon": me_lon + step_of[b]},
            device_id_type=MESH,
        )

    def lat_copy(a, k):
        f, d = fields[k], depth[k]
        src = top if a == 0 else bottom - d
        dst = bottom if a == 0 else top - d
        return pltpu.make_async_remote_copy(
            src_ref=f.at[src:src + d, left:right],
            dst_ref=f.at[dst:dst + d, left:right],
            send_sem=lat_sems.at[0, a, k],
            recv_sem=lat_sems.at[1, 1 - a, k],
            device_id={"lat": me_lat + step_of[a], "lon": me_lon},
            device_id_type=MESH,
        )

    for a in range(2):
        for b in range(2):
            @pl.when(has_lat[a] & has_lon[b])
            def _():
                corner_copy(a, b).start()
    for b in range(2):
        @pl.when(has_lon[b])
        def _():
            lon_copy(b).start()
    for a in range(2):
        @pl.when(has_lat[a])
        def _():
            for k in range(3):
                lat_copy(a, k).start()

    for a in range(2):
        for b in range(2):
            @pl.when(has_lat[a] & has_lon[b])
            def _():
                corner_copy(1 - a, 1 - b).wait_recv()
                corner_copy(a, b).wait_send()
                for k, (which, i, j) in enumerate(cells):
                    r = top - 1 - i if a == 0 else bottom + i
                    s = left - 1 - j if b == 0 else right + j
                    fields[which][r, s:s + 1] = corner_recv[2 * a + b, k:k + 1]
    for b in range(2):
        @pl.when(has_lon[b])
        def _():
            lon_copy(1 - b).wait_recv()
            lon_copy(b).wait_send()
            base = 0
            for f, d in zip(fields, depth):
                start = left - d if b == 0 else right
                for r in range(rows):
                    f[top + r, start:start + d] = lon_recv[b, base + r * d:base + (r + 1) * d]
                base += rows * d
    for a in range(2):
        @pl.when(has_lat[a])
        def _():
            for k in range(3):
                lat_copy(1 - a, k).wait_recv()
                lat_copy(a, k).wait_send()

    now, old = p, e
    for step in range(STEPS):
        margin = STEPS - 1 - step
        lo, hi = left - margin, right + margin
        last = step == STEPS - 1

        def one_row(r, total, now=now, old=old, lo=lo, hi=hi, last=last):
            middle = now[r, lo:hi]
            spread = (
                now[r - 1, lo:hi] + now[r + 1, lo:hi]
                + now[r, lo - 1:hi - 1] + now[r, lo + 1:hi + 1] - 4.0 * middle
            )
            later = 2.0 * middle - old[r, lo:hi] + c[r, lo:hi] * spread
            if not last:
                old[r, lo:hi] = later
            else:
                end[r - top] = later
                total = total + later
                here[r - top] = total
            return total

        start = jnp.zeros((cols, p.shape[2]), p.dtype) if last else 0
        total = lax.fori_loop(top - margin, bottom + margin, one_row, start, unroll=2)
        now, old = old, now
    below[...] = total

    def total_copy(j):
        return pltpu.make_async_remote_copy(
            src_ref=below,
            dst_ref=totals.at[me_lat],
            send_sem=total_send_sem.at[j],
            recv_sem=total_recv_sem.at[me_lat],
            device_id={"lat": j, "lon": me_lon},
            device_id_type=MESH,
        )

    def total_arrival(j):
        return pltpu.make_async_remote_copy(
            src_ref=below,
            dst_ref=totals.at[j],
            send_sem=total_send_sem.at[j],
            recv_sem=total_recv_sem.at[j],
            device_id={"lat": j, "lon": me_lon},
            device_id_type=MESH,
        )

    for j in reversed(range(1, n_lat)):
        @pl.when(me_lat < j)
        def _():
            total_copy(j).start()
    def arrive(j, acc):
        total_arrival(j).wait_recv()
        return acc + totals[j]

    before[...] = lax.fori_loop(0, me_lat, arrive, jnp.zeros((cols, p.shape[2]), p.dtype))
    for j in range(1, n_lat):
        @pl.when(me_lat < j)
        def _():
            total_copy(j).wait_send()


def finish(scale, here, end, before, pot_out, end_out, pot, sems):
    rows = here.shape[0]
    end_copy = pltpu.make_async_copy(end, end_out, sems.at[0])
    end_copy.start()
    half = rows // 2
    copies = []
    for part in range(2):
        for r in range(part * half, (part + 1) * half):
            pot[r] = (here[r] + before[...]) * scale
        span = pl.ds(part * half, half)
        copy = pltpu.make_async_copy(pot.at[span], pot_out.at[span], sems.at[1 + part])
        copy.start()
        copies.append(copy)
    for copy in copies:
        copy.wait()
    end_copy.wait()


def on_device(n_lat, n_lon, pressure, earlier, speed_square):
    rows, cols, members = pressure.shape
    packed = rows * (3 * STEPS - 2)
    corner_rows = -(-len(corner_cells()) // 8) * 8
    f32 = jnp.float32
    wide = pltpu.VMEM((rows + 2 * STEPS, cols + 2 * PAD, members), f32)
    any_space = pl.BlockSpec(memory_space=pl.ANY)
    dma = pltpu.SemaphoreType.DMA
    vmem = pltpu.MemorySpace.VMEM
    here, end, before = pl.pallas_call(
        functools.partial(kernel, n_lat, n_lon),
        out_shape=[
            vmem(pressure.shape, f32), vmem(pressure.shape, f32), vmem((cols, members), f32)
        ],
        in_specs=[any_space] * 3,
        out_specs=[pl.BlockSpec(memory_space=vmem)] * 3,
        scratch_shapes=[
            wide, wide, wide,
            pltpu.VMEM((2, packed, members), f32),
            pltpu.VMEM((2, packed, members), f32),
            pltpu.VMEM((4, corner_rows, members), f32),
            pltpu.VMEM((4, corner_rows, members), f32),
            pltpu.VMEM((n_lat, cols, members), f32),
            pltpu.VMEM((cols, members), f32),
            dma((3,)), dma((2, 2, 3)), dma((2, 2)), dma((2, 4)),
            dma((n_lat,)), dma((n_lat,)),
        ],
        compiler_params=pltpu.CompilerParams(collective_id=0, has_side_effects=True),
        name="waves",
    )(pressure, earlier, speed_square)
    return pl.pallas_call(
        functools.partial(finish, 1.0 / (rows * n_lat)),
        out_shape=[jax.ShapeDtypeStruct(pressure.shape, f32)] * 2,
        in_specs=[pl.BlockSpec(memory_space=vmem)] * 3,
        out_specs=[any_space] * 2,
        scratch_shapes=[pltpu.VMEM(pressure.shape, f32), dma((3,))],
        name="finish",
    )(*(pltpu.with_memory_space_constraint(x, vmem) for x in (here, end, before)))


def solution(mesh):
    spec = P("lat", "lon", None)
    body = functools.partial(on_device, mesh.shape["lat"], mesh.shape["lon"])
    return jax.shard_map(
        body, mesh=mesh, in_specs=(spec,) * 3, out_specs=(spec,) * 2, check_vma=False
    )
```

```python
import functools

import jax
import jax.numpy as jnp
from jax import lax
from jax.experimental import pallas as pl
from jax.experimental.pallas import tpu as pltpu
from jax.sharding import PartitionSpec as P

STEPS = 4
PAD = 8
MESH = pl.DeviceIdType.MESH


def corner_cells():
    cells = [(0, i, 0) for i in range(STEPS - 1)] + [(0, 0, j) for j in range(1, STEPS - 1)]
    for array in (1, 2):
        cells += [(array, i, j) for i in range(STEPS - 2) for j in range(STEPS - 2 - i)]
    return cells


def kernel(
    n_lat, n_lon, p_in, e_in, c_in, here, end, before,
    p, e, c, lon_send, lon_recv, corner_send, corner_recv,
    p_recv, e_recv, c_recv, totals, below,
    load_sem, ready_sem, lat_sems, lon_sems, corner_sems, total_send_sem, total_recv_sem,
):
    rows, cols = p_in.shape[0], p_in.shape[1]
    fields = (p, e, c)
    lat_depth = (STEPS - 2, STEPS - 1, STEPS - 1)
    lon_depth = (STEPS - 2, STEPS - 1, STEPS - 2)
    received = (p_recv, e_recv, c_recv)
    top, left = STEPS, PAD
    bottom, right = top + rows, left + cols
    me_lat, me_lon = lax.axis_index("lat"), lax.axis_index("lon")
    has_lat = (me_lat > 0, me_lat < n_lat - 1)
    has_lon = (me_lon > 0, me_lon < n_lon - 1)
    step_of = (-1, 1)

    loads = []
    for k, (src, dst) in enumerate(zip((p_in, e_in, c_in), fields)):
        copy = pltpu.make_async_copy(src, dst.at[top:bottom, left:right], load_sem.at[k])
        copy.start()
        loads.append(copy)

    barrier = pltpu.get_barrier_semaphore()

    def greet(lat, lon):
        pl.semaphore_signal(
            barrier, inc=1, device_id={"lat": lat, "lon": lon}, device_id_type=MESH
        )

    for b in range(2):
        @pl.when(has_lon[b])
        def _():
            greet(me_lat, me_lon + step_of[b])
    for j in range(n_lat):
        @pl.when(me_lat != j)
        def _():
            greet(j, me_lon)

    zero = jnp.int32(0)
    one = jnp.int32(1)
    count_lat = sum(jnp.where(h, one, zero) for h in has_lat)
    count_lon = sum(jnp.where(h, one, zero) for h in has_lon)
    peers = n_lat - 1 + count_lon

    width = p.shape[2]
    for r in (top - 1, bottom):
        p[r] = jnp.zeros(p.shape[1:], p.dtype)
    for s in (0, right):
        p[top:bottom, s:s + PAD] = jnp.zeros((rows, PAD, width), p.dtype)
    for a in range(2):
        @pl.when(jnp.logical_not(has_lat[a]))
        def _():
            for f in fields:
                start = 0 if a == 0 else bottom
                f[start:start + STEPS] = jnp.zeros((STEPS,) + f.shape[1:], f.dtype)
    for b in range(2):
        @pl.when(jnp.logical_not(has_lon[b]))
        def _():
            for f in fields:
                start = 0 if b == 0 else right
                f[:, start:start + PAD] = jnp.zeros((f.shape[0], PAD, f.shape[2]), f.dtype)

    for copy in loads:
        copy.wait()

    def advance(now, old, r, lo, hi):
        middle = now[r, lo:hi]
        spread = (
            now[r - 1, lo:hi] + now[r + 1, lo:hi]
            + now[r, lo - 1:hi - 1] + now[r, lo + 1:hi + 1] - 4.0 * middle
        )
        return 2.0 * middle - old[r, lo:hi] + c[r, lo:hi] * spread

    def first_row(r, carry):
        e[r, left:right] = advance(p, e, r, left, right)
        return carry

    lax.fori_loop(top, bottom, first_row, 0, unroll=2)

    for b in range(2):
        @pl.when(has_lon[b])
        def _():
            base = 0
            for f, d in zip(fields, lon_depth):
                start = left if b == 0 else right - d
                for r in range(rows):
                    lon_send[b, base + r * d:base + (r + 1) * d] = f[top + r, start:start + d]
                base += rows * d
            s = left + STEPS - 2 if b == 0 else right - STEPS + 1
            for k, r in enumerate((top, bottom - 1)):
                lon_send[b, base + k:base + k + 1] = c[r, s:s + 1]
    cells = corner_cells()
    for a in range(2):
        for b in range(2):
            @pl.when(has_lat[a] & has_lon[b])
            def _():
                for k, (which, i, j) in enumerate(cells):
                    r = top + i if a == 0 else bottom - 1 - i
                    s = left + j if b == 0 else right - 1 - j
                    corner_send[2 * a + b, k:k + 1] = fields[which][r, s:s + 1]

    pl.semaphore_wait(barrier, peers)

    def corner_copy(a, b):
        return pltpu.make_async_remote_copy(
            src_ref=corner_send.at[2 * a + b],
            dst_ref=corner_recv.at[2 * (1 - a) + 1 - b],
            send_sem=corner_sems.at[0, 2 * a + b],
            recv_sem=corner_sems.at[1, 2 * (1 - a) + 1 - b],
            device_id={"lat": me_lat + step_of[a], "lon": me_lon + step_of[b]},
            device_id_type=MESH,
        )

    def lon_copy(b):
        return pltpu.make_async_remote_copy(
            src_ref=lon_send.at[b],
            dst_ref=lon_recv.at[1 - b],
            send_sem=lon_sems.at[0, b],
            recv_sem=lon_sems.at[1, 1 - b],
            device_id={"lat": me_lat, "lon": me_lon + step_of[b]},
            device_id_type=MESH,
        )

    def lat_copy(a, k):
        f, d = fields[k], lat_depth[k]
        src = top if a == 0 else bottom - d
        return pltpu.make_async_remote_copy(
            src_ref=f.at[src:src + d, left:right],
            dst_ref=received[k].at[1 - a],
            send_sem=lat_sems.at[0, a, k],
            recv_sem=lat_sems.at[1, 1 - a, k],
            device_id={"lat": me_lat + step_of[a], "lon": me_lon},
            device_id_type=MESH,
        )

    for b in range(2):
        @pl.when(has_lon[b])
        def _():
            lon_copy(b).start()
    for a in range(2):
        @pl.when(has_lat[a])
        def _():
            for k in range(3):
                lat_copy(a, k).start()
    for a in range(2):
        @pl.when(has_lat[a])
        def _():
            pl.semaphore_signal(
                ready_sem, inc=1, device_id={"lat": me_lat + step_of[a], "lon": me_lon},
                device_id_type=MESH,
            )
    pl.semaphore_wait(ready_sem, count_lat)
    for a in range(2):
        for b in range(2):
            @pl.when(has_lat[a] & has_lon[b])
            def _():
                corner_copy(a, b).start()

    for a in range(2):
        for b in range(2):
            @pl.when(has_lat[a] & has_lon[b])
            def _():
                corner_copy(1 - a, 1 - b).wait_recv()
                corner_copy(a, b).wait_send()
                for k, (which, i, j) in enumerate(cells):
                    r = top - 1 - i if a == 0 else bottom + i
                    s = left - 1 - j if b == 0 else right + j
                    fields[which][r, s:s + 1] = corner_recv[2 * a + b, k:k + 1]
    for b in range(2):
        @pl.when(has_lon[b])
        def _():
            lon_copy(1 - b).wait_recv()
            lon_copy(b).wait_send()
            base = 0
            for f, d in zip(fields, lon_depth):
                start = left - d if b == 0 else right
                for r in range(rows):
                    f[top + r, start:start + d] = lon_recv[b, base + r * d:base + (r + 1) * d]
                base += rows * d
            s = left - STEPS + 1 if b == 0 else right + STEPS - 2
            for k, r in enumerate((top, bottom - 1)):
                c[r, s:s + 1] = lon_recv[b, base + k:base + k + 1]
    for a in range(2):
        @pl.when(has_lat[a])
        def _():
            for k in range(3):
                lat_copy(1 - a, k).wait_recv()
                lat_copy(a, k).wait_send()
                d = lat_depth[k]
                dst = top - d if a == 0 else bottom
                fields[k][dst:dst + d, left:right] = received[k][a]

    def add(r, lo, hi, r_from, shift):
        e[r, lo:hi] = e[r, lo:hi] + c[r, lo:hi] * p[r_from, lo + shift:hi + shift]

    for near, far in ((top, top - 1), (bottom - 1, bottom)):
        add(near, left - 3, right + 3, far, 0)
        add(far, left - 2, right + 2, near, 0)

    def lon_edges(r, carry):
        add(r, left, left + 1, r, -1)
        add(r, left - 1, left, r, 1)
        add(r, right - 1, right, r, 1)
        add(r, right, right + 1, r, -1)
        return carry

    lax.fori_loop(top - 3, bottom + 3, lon_edges, 0, unroll=2)

    now, old = e, p
    for step in range(1, STEPS):
        margin = STEPS - 1 - step
        lo, hi = left - margin, right + margin
        last = step == STEPS - 1

        def one_row(r, total, now=now, old=old, lo=lo, hi=hi, last=last):
            later = advance(now, old, r, lo, hi)
            if not last:
                old[r, lo:hi] = later
            else:
                end[r - top] = later
                total = total + later
                here[r - top] = total
            return total

        start = jnp.zeros((cols, width), p.dtype) if last else 0
        total = lax.fori_loop(top - margin, bottom + margin, one_row, start, unroll=2)
        now, old = old, now
    below[...] = total

    def total_copy(j):
        return pltpu.make_async_remote_copy(
            src_ref=below,
            dst_ref=totals.at[me_lat],
            send_sem=total_send_sem.at[j],
            recv_sem=total_recv_sem.at[me_lat],
            device_id={"lat": j, "lon": me_lon},
            device_id_type=MESH,
        )

    def total_arrival(j):
        return pltpu.make_async_remote_copy(
            src_ref=below,
            dst_ref=totals.at[j],
            send_sem=total_send_sem.at[j],
            recv_sem=total_recv_sem.at[j],
            device_id={"lat": j, "lon": me_lon},
            device_id_type=MESH,
        )

    for j in reversed(range(1, n_lat)):
        @pl.when(me_lat < j)
        def _():
            total_copy(j).start()
    def arrive(j, acc):
        total_arrival(j).wait_recv()
        return acc + totals[j]

    before[...] = lax.fori_loop(0, me_lat, arrive, jnp.zeros((cols, p.shape[2]), p.dtype))
    for j in range(1, n_lat):
        @pl.when(me_lat < j)
        def _():
            total_copy(j).wait_send()


def finish(scale, here, end, before, pot_out, end_out, pot, sems):
    rows = here.shape[0]
    end_copy = pltpu.make_async_copy(end, end_out, sems.at[0])
    end_copy.start()
    half = rows // 2
    copies = []
    for part in range(2):
        for r in range(part * half, (part + 1) * half):
            pot[r] = (here[r] + before[...]) * scale
        span = pl.ds(part * half, half)
        copy = pltpu.make_async_copy(pot.at[span], pot_out.at[span], sems.at[1 + part])
        copy.start()
        copies.append(copy)
    for copy in copies:
        copy.wait()
    end_copy.wait()


def on_device(n_lat, n_lon, pressure, earlier, speed_square):
    rows, cols, members = pressure.shape
    packed = -(-(rows * (3 * STEPS - 5) + 2) // 8) * 8
    corner_rows = -(-len(corner_cells()) // 8) * 8
    f32 = jnp.float32
    wide = pltpu.VMEM((rows + 2 * STEPS, cols + 2 * PAD, members), f32)
    any_space = pl.BlockSpec(memory_space=pl.ANY)
    dma = pltpu.SemaphoreType.DMA
    vmem = pltpu.MemorySpace.VMEM
    here, end, before = pl.pallas_call(
        functools.partial(kernel, n_lat, n_lon),
        out_shape=[
            vmem(pressure.shape, f32), vmem(pressure.shape, f32), vmem((cols, members), f32)
        ],
        in_specs=[any_space] * 3,
        out_specs=[pl.BlockSpec(memory_space=vmem)] * 3,
        scratch_shapes=[
            wide, wide, wide,
            pltpu.VMEM((2, packed, members), f32),
            pltpu.VMEM((2, packed, members), f32),
            pltpu.VMEM((4, corner_rows, members), f32),
            pltpu.VMEM((4, corner_rows, members), f32),
            pltpu.VMEM((2, STEPS - 2, cols, members), f32),
            pltpu.VMEM((2, STEPS - 1, cols, members), f32),
            pltpu.VMEM((2, STEPS - 1, cols, members), f32),
            pltpu.VMEM((n_lat, cols, members), f32),
            pltpu.VMEM((cols, members), f32),
            dma((3,)), pltpu.SemaphoreType.REGULAR, dma((2, 2, 3)), dma((2, 2)), dma((2, 4)),
            dma((n_lat,)), dma((n_lat,)),
        ],
        compiler_params=pltpu.CompilerParams(collective_id=0, has_side_effects=True),
        name="waves",
    )(pressure, earlier, speed_square)
    return pl.pallas_call(
        functools.partial(finish, 1.0 / (rows * n_lat)),
        out_shape=[jax.ShapeDtypeStruct(pressure.shape, f32)] * 2,
        in_specs=[pl.BlockSpec(memory_space=vmem)] * 3,
        out_specs=[any_space] * 2,
        scratch_shapes=[pltpu.VMEM(pressure.shape, f32), dma((3,))],
        name="finish",
    )(*(pltpu.with_memory_space_constraint(x, vmem) for x in (here, end, before)))


def solution(mesh):
    spec = P("lat", "lon", None)
    body = functools.partial(on_device, mesh.shape["lat"], mesh.shape["lon"])
    return jax.shard_map(
        body, mesh=mesh, in_specs=(spec,) * 3, out_specs=(spec,) * 2, check_vma=False
    )
```

```python
import functools

import jax
import jax.numpy as jnp
from jax import lax
from jax.experimental import pallas as pl
from jax.experimental.pallas import tpu as pltpu
from jax.sharding import PartitionSpec as P

STEPS = 4
PAD = 8
MESH = pl.DeviceIdType.MESH


def corner_cells():
    cells = [(0, i, 0) for i in range(STEPS - 1)] + [(0, 0, j) for j in range(1, STEPS - 1)]
    for array in (1, 2):
        cells += [(array, i, j) for i in range(STEPS - 2) for j in range(STEPS - 2 - i)]
    return cells


def kernel(
    n_lat, n_lon, p_in, e_in, c_in, here, end, before,
    p, e, c, lon_send, lon_recv, corner_send, corner_recv,
    p_recv, e_recv, c_recv, totals, below,
    load_sem, ready_sem, lat_sems, lon_sems, corner_sems, total_send_sem, total_recv_sem,
):
    rows, cols = p_in.shape[0], p_in.shape[1]
    fields = (p, e, c)
    lat_depth = (STEPS - 2, STEPS - 1, STEPS - 1)
    lon_depth = (STEPS - 2, STEPS - 1, STEPS - 2)
    received = (p_recv, e_recv, c_recv)
    top, left = STEPS, PAD
    bottom, right = top + rows, left + cols
    me_lat, me_lon = lax.axis_index("lat"), lax.axis_index("lon")
    has_lat = (me_lat > 0, me_lat < n_lat - 1)
    has_lon = (me_lon > 0, me_lon < n_lon - 1)
    step_of = (-1, 1)

    loads = []
    for k, (src, dst) in enumerate(zip((p_in, e_in, c_in), fields)):
        copy = pltpu.make_async_copy(src, dst.at[top:bottom, left:right], load_sem.at[k])
        copy.start()
        loads.append(copy)

    barrier = pltpu.get_barrier_semaphore()

    def greet(lat, lon):
        pl.semaphore_signal(
            barrier, inc=1, device_id={"lat": lat, "lon": lon}, device_id_type=MESH
        )

    for b in range(2):
        @pl.when(has_lon[b])
        def _():
            greet(me_lat, me_lon + step_of[b])
    for j in range(n_lat):
        @pl.when(me_lat != j)
        def _():
            greet(j, me_lon)

    zero = jnp.int32(0)
    one = jnp.int32(1)
    count_lat = sum(jnp.where(h, one, zero) for h in has_lat)
    count_lon = sum(jnp.where(h, one, zero) for h in has_lon)
    peers = n_lat - 1 + count_lon

    width = p.shape[2]
    for r in (top - 1, bottom):
        p[r] = jnp.zeros(p.shape[1:], p.dtype)
    for s in (0, right):
        p[top:bottom, s:s + PAD] = jnp.zeros((rows, PAD, width), p.dtype)
    for a in range(2):
        @pl.when(jnp.logical_not(has_lat[a]))
        def _():
            for f in fields:
                start = 0 if a == 0 else bottom
                f[start:start + STEPS] = jnp.zeros((STEPS,) + f.shape[1:], f.dtype)
    for b in range(2):
        @pl.when(jnp.logical_not(has_lon[b]))
        def _():
            for f in fields:
                start = 0 if b == 0 else right
                f[:, start:start + PAD] = jnp.zeros((f.shape[0], PAD, f.shape[2]), f.dtype)

    for copy in loads:
        copy.wait()

    def advance(now, old, r, lo, hi):
        middle = now[r, lo:hi]
        spread = (
            now[r - 1, lo:hi] + now[r + 1, lo:hi]
            + now[r, lo - 1:hi - 1] + now[r, lo + 1:hi + 1] - 4.0 * middle
        )
        return 2.0 * middle - old[r, lo:hi] + c[r, lo:hi] * spread

    def first_row(r, carry):
        e[r, left:right] = advance(p, e, r, left, right)
        return carry

    lax.fori_loop(top, bottom, first_row, 0, unroll=4)

    for b in range(2):
        @pl.when(has_lon[b])
        def _():
            base = 0
            for f, d in zip(fields, lon_depth):
                start = left if b == 0 else right - d
                for r in range(rows):
                    lon_send[b, base + r * d:base + (r + 1) * d] = f[top + r, start:start + d]
                base += rows * d
            s = left + STEPS - 2 if b == 0 else right - STEPS + 1
            for k, r in enumerate((top, bottom - 1)):
                lon_send[b, base + k:base + k + 1] = c[r, s:s + 1]
    cells = corner_cells()
    for a in range(2):
        for b in range(2):
            @pl.when(has_lat[a] & has_lon[b])
            def _():
                for k, (which, i, j) in enumerate(cells):
                    r = top + i if a == 0 else bottom - 1 - i
                    s = left + j if b == 0 else right - 1 - j
                    corner_send[2 * a + b, k:k + 1] = fields[which][r, s:s + 1]

    pl.semaphore_wait(barrier, peers)

    def corner_copy(a, b):
        return pltpu.make_async_remote_copy(
            src_ref=corner_send.at[2 * a + b],
            dst_ref=corner_recv.at[2 * (1 - a) + 1 - b],
            send_sem=corner_sems.at[0, 2 * a + b],
            recv_sem=corner_sems.at[1, 2 * (1 - a) + 1 - b],
            device_id={"lat": me_lat + step_of[a], "lon": me_lon + step_of[b]},
            device_id_type=MESH,
        )

    def lon_copy(b):
        return pltpu.make_async_remote_copy(
            src_ref=lon_send.at[b],
            dst_ref=lon_recv.at[1 - b],
            send_sem=lon_sems.at[0, b],
            recv_sem=lon_sems.at[1, 1 - b],
            device_id={"lat": me_lat, "lon": me_lon + step_of[b]},
            device_id_type=MESH,
        )

    def lat_copy(a, k):
        f, d = fields[k], lat_depth[k]
        src = top if a == 0 else bottom - d
        return pltpu.make_async_remote_copy(
            src_ref=f.at[src:src + d, left:right],
            dst_ref=received[k].at[1 - a],
            send_sem=lat_sems.at[0, a, k],
            recv_sem=lat_sems.at[1, 1 - a, k],
            device_id={"lat": me_lat + step_of[a], "lon": me_lon},
            device_id_type=MESH,
        )

    for b in range(2):
        @pl.when(has_lon[b])
        def _():
            lon_copy(b).start()
    for a in range(2):
        @pl.when(has_lat[a])
        def _():
            for k in range(3):
                lat_copy(a, k).start()
    for a in range(2):
        @pl.when(has_lat[a])
        def _():
            pl.semaphore_signal(
                ready_sem, inc=1, device_id={"lat": me_lat + step_of[a], "lon": me_lon},
                device_id_type=MESH,
            )
    pl.semaphore_wait(ready_sem, count_lat)
    for a in range(2):
        for b in range(2):
            @pl.when(has_lat[a] & has_lon[b])
            def _():
                corner_copy(a, b).start()

    unroll = 4

    def put(now, old, r, lo, hi, last):
        later = advance(now, old, r, lo, hi)
        if last:
            end[r - top, lo - left:hi - left] = later
        else:
            old[r, lo:hi] = later

    now, old = e, p
    for step in range(1, STEPS):
        inside = step + 1

        def inner_row(r, carry, now=now, old=old, inside=inside, last=step == STEPS - 1):
            put(now, old, r, left + inside, right - inside, last)
            return carry

        lax.fori_loop(top + inside, bottom - inside, inner_row, 0, unroll=unroll)
        now, old = old, now

    for a in range(2):
        for b in range(2):
            @pl.when(has_lat[a] & has_lon[b])
            def _():
                corner_copy(1 - a, 1 - b).wait_recv()
                corner_copy(a, b).wait_send()
                for k, (which, i, j) in enumerate(cells):
                    r = top - 1 - i if a == 0 else bottom + i
                    s = left - 1 - j if b == 0 else right + j
                    fields[which][r, s:s + 1] = corner_recv[2 * a + b, k:k + 1]
    for a in range(2):
        @pl.when(has_lat[a])
        def _():
            for k in range(3):
                lat_copy(1 - a, k).wait_recv()
                lat_copy(a, k).wait_send()
                d = lat_depth[k]
                dst = top - d if a == 0 else bottom
                fields[k][dst:dst + d, left:right] = received[k][a]

    for b in range(2):
        @pl.when(has_lon[b])
        def _():
            lon_copy(1 - b).wait_recv()
            lon_copy(b).wait_send()
            base = 0
            for f, d in zip(fields, lon_depth):
                start = left - d if b == 0 else right
                for r in range(rows):
                    f[top + r, start:start + d] = lon_recv[b, base + r * d:base + (r + 1) * d]
                base += rows * d
            s = left - STEPS + 1 if b == 0 else right + STEPS - 2
            for k, r in enumerate((top, bottom - 1)):
                c[r, s:s + 1] = lon_recv[b, base + k:base + k + 1]

    def add(r, lo, hi, r_from, shift):
        e[r, lo:hi] = e[r, lo:hi] + c[r, lo:hi] * p[r_from, lo + shift:hi + shift]

    for near, far in ((top, top - 1), (bottom - 1, bottom)):
        add(near, left - 3, right + 3, far, 0)
        add(far, left - 2, right + 2, near, 0)

    def lon_edges(r, carry):
        add(r, left, left + 1, r, -1)
        add(r, left - 1, left, r, 1)
        add(r, right - 1, right, r, 1)
        add(r, right, right + 1, r, -1)
        return carry

    lax.fori_loop(top - 3, bottom + 3, lon_edges, 0, unroll=2)

    now, old = e, p
    for step in range(1, STEPS):
        margin, inside, last = STEPS - 1 - step, step + 1, step == STEPS - 1
        lo, hi = left - margin, right + margin
        for r in list(range(top - margin, top + inside)) + list(
            range(bottom - inside, bottom + margin)
        ):
            put(now, old, r, lo, hi, last)

        def side_row(r, carry, now=now, old=old, lo=lo, hi=hi, inside=inside, last=last):
            put(now, old, r, lo, left + inside, last)
            put(now, old, r, right - inside, hi, last)
            return carry

        lax.fori_loop(top + inside, bottom - inside, side_row, 0, unroll=unroll)
        now, old = old, now
    parts = [end[r] for r in range(4)]
    for r in range(4, rows):
        parts[r % 4] = parts[r % 4] + end[r]
    total = (parts[0] + parts[1]) + (parts[2] + parts[3])
    below[...] = total

    def total_copy(j):
        return pltpu.make_async_remote_copy(
            src_ref=below,
            dst_ref=totals.at[me_lat],
            send_sem=total_send_sem.at[j],
            recv_sem=total_recv_sem.at[me_lat],
            device_id={"lat": j, "lon": me_lon},
            device_id_type=MESH,
        )

    def total_arrival(j):
        return pltpu.make_async_remote_copy(
            src_ref=below,
            dst_ref=totals.at[j],
            send_sem=total_send_sem.at[j],
            recv_sem=total_recv_sem.at[j],
            device_id={"lat": j, "lon": me_lon},
            device_id_type=MESH,
        )

    for j in reversed(range(1, n_lat)):
        @pl.when(me_lat < j)
        def _():
            total_copy(j).start()
    def sum_row(r, running):
        running = running + end[r]
        here[r] = running
        return running

    lax.fori_loop(0, rows, sum_row, jnp.zeros((cols, width), p.dtype), unroll=4)

    def arrive(j, acc):
        total_arrival(j).wait_recv()
        return acc + totals[j]

    before[...] = lax.fori_loop(0, me_lat, arrive, jnp.zeros((cols, p.shape[2]), p.dtype))
    for j in range(1, n_lat):
        @pl.when(me_lat < j)
        def _():
            total_copy(j).wait_send()


def finish(scale, here, end, before, pot_out, end_out, pot, sems):
    rows = here.shape[0]
    end_copy = pltpu.make_async_copy(end, end_out, sems.at[0])
    end_copy.start()
    half = rows // 2
    copies = []
    for part in range(2):
        for r in range(part * half, (part + 1) * half):
            pot[r] = (here[r] + before[...]) * scale
        span = pl.ds(part * half, half)
        copy = pltpu.make_async_copy(pot.at[span], pot_out.at[span], sems.at[1 + part])
        copy.start()
        copies.append(copy)
    for copy in copies:
        copy.wait()
    end_copy.wait()


def on_device(n_lat, n_lon, pressure, earlier, speed_square):
    rows, cols, members = pressure.shape
    packed = -(-(rows * (3 * STEPS - 5) + 2) // 8) * 8
    corner_rows = -(-len(corner_cells()) // 8) * 8
    f32 = jnp.float32
    wide = pltpu.VMEM((rows + 2 * STEPS, cols + 2 * PAD, members), f32)
    any_space = pl.BlockSpec(memory_space=pl.ANY)
    dma = pltpu.SemaphoreType.DMA
    vmem = pltpu.MemorySpace.VMEM
    here, end, before = pl.pallas_call(
        functools.partial(kernel, n_lat, n_lon),
        out_shape=[
            vmem(pressure.shape, f32), vmem(pressure.shape, f32), vmem((cols, members), f32)
        ],
        in_specs=[any_space] * 3,
        out_specs=[pl.BlockSpec(memory_space=vmem)] * 3,
        scratch_shapes=[
            wide, wide, wide,
            pltpu.VMEM((2, packed, members), f32),
            pltpu.VMEM((2, packed, members), f32),
            pltpu.VMEM((4, corner_rows, members), f32),
            pltpu.VMEM((4, corner_rows, members), f32),
            pltpu.VMEM((2, STEPS - 2, cols, members), f32),
            pltpu.VMEM((2, STEPS - 1, cols, members), f32),
            pltpu.VMEM((2, STEPS - 1, cols, members), f32),
            pltpu.VMEM((n_lat, cols, members), f32),
            pltpu.VMEM((cols, members), f32),
            dma((3,)), pltpu.SemaphoreType.REGULAR, dma((2, 2, 3)), dma((2, 2)), dma((2, 4)),
            dma((n_lat,)), dma((n_lat,)),
        ],
        compiler_params=pltpu.CompilerParams(collective_id=0, has_side_effects=True),
        name="waves",
    )(pressure, earlier, speed_square)
    return pl.pallas_call(
        functools.partial(finish, 1.0 / (rows * n_lat)),
        out_shape=[jax.ShapeDtypeStruct(pressure.shape, f32)] * 2,
        in_specs=[pl.BlockSpec(memory_space=vmem)] * 3,
        out_specs=[any_space] * 2,
        scratch_shapes=[pltpu.VMEM(pressure.shape, f32), dma((3,))],
        name="finish",
    )(*(pltpu.with_memory_space_constraint(x, vmem) for x in (here, end, before)))


def solution(mesh):
    spec = P("lat", "lon", None)
    body = functools.partial(on_device, mesh.shape["lat"], mesh.shape["lon"])
    return jax.shard_map(
        body, mesh=mesh, in_specs=(spec,) * 3, out_specs=(spec,) * 2, check_vma=False
    )
```
